32 devices in a mesh: seq: 8 (over z, x), tp: 4 (over y, core).
Axes of the slice: x: 2, y: 2, z: 4, core: 2. Of those that a mesh axis runs over, the one named last changes fastest.
Arguments:
- layer_in: bfloat16 [6144, 2048], P('seq', 'tp'), may hold values from -6 to 6
- attn_gain: float32 [2048], replicated, may hold values from 0.1 to 1.9
- qkv_weight: bfloat16 [3, 2048, 1024], P(None, None, 'tp'), may hold values from -0.125 to 0.125
- log_decay: float32 [8, 6144], P('tp', 'seq'), may hold values from -0.1 to 0
- write_rate: float32 [8, 6144], P('tp', 'seq'), may hold values from 0 to 0.9
- head_gain: float32 [128], replicated, may hold values from 0.1 to 1.9
- out_weight: bfloat16 [1024, 2048], P('tp'), may hold values from -0.1875 to 0.1875
- ffn_gain: float32 [2048], replicated, may hold values from 0.1 to 1.9
- gate_weight: bfloat16 [2048, 2560], P(None, 'tp'), may hold values from -0.125 to 0.125
- up_weight: bfloat16 [2048, 2560], P(None, 'tp'), may hold values from -0.125 to 0.125
- down_weight: bfloat16 [2560, 2048], P('tp'), may hold values from -0.125 to 0.125
Outputs:
- layer_out: bfloat16 [6144, 2048], P('seq', 'tp')
The draws below stay inside these ranges and needn't reach their ends.
All inputs are finite; a program needn't handle non-finite values.
Results may differ from the reference program's by a relative error of at most 0.014.
Values may be sent and summed in bfloat16 or wider, within the bound.
No kernel may reach another device: no remote copies, remote signals or barrier semaphores. Data moves between devices by JAX's collectives and lax.ppermute only.
A program may use at most 128 MiB of HBM per device.

```python
import math
import jax
import jax.numpy as jnp
from jax import lax

D = 2048
HEADS = 8
DK = 128
FF = 2560
TOK_DEV = 768
SEQLEN = 6144
N_TP = 4


def head_kinds(key):
    kind_key = jax.random.fold_in(key, 101)
    order_key = jax.random.fold_in(key, 102)
    slow_share = 0.5
    slow_heads = jax.random.uniform(kind_key, (HEADS,)) < slow_share
    order = jax.random.permutation(order_key, HEADS)
    slow_heads = slow_heads.at[order[0]].set(True)
    slow_heads = slow_heads.at[order[1]].set(False)
    return slow_heads


def draw_log_decay(key, part):
    slow_heads = head_kinds(key)
    slow_rate = jax.random.uniform(jax.random.fold_in(key, 1), (HEADS, 1), minval=0.2, maxval=0.6) / SEQLEN
    fast_rate = jax.random.uniform(jax.random.fold_in(key, 2), (HEADS, 1), minval=1.0 / 50.0, maxval=1.0 / 30.0)
    base_rate = jnp.where(slow_heads[:, None], slow_rate, fast_rate)
    blocks = SEQLEN // TOK_DEV
    device_scale = jnp.exp(jax.random.uniform(jax.random.fold_in(key, 3), (HEADS, blocks, 1), minval=math.log(0.5), maxval=math.log(2.0)))
    device_scale = jnp.broadcast_to(device_scale, (HEADS, blocks, TOK_DEV)).reshape(HEADS, SEQLEN)
    jitter = jax.random.uniform(jax.random.fold_in(key, 4), (HEADS, SEQLEN), minval=0.5, maxval=1.5)
    return -(base_rate * device_scale * jitter).astype(jnp.float32)


def draw_write_rate(key, part):
    slow_heads = head_kinds(key)
    slow_rate = jax.random.uniform(jax.random.fold_in(key, 5), (HEADS, SEQLEN), minval=0.05, maxval=0.4) * DK / SEQLEN
    fast_rate = jax.random.uniform(jax.random.fold_in(key, 6), (HEADS, SEQLEN), minval=0.1, maxval=0.9)
    chosen = jnp.where(slow_heads[:, None], slow_rate, fast_rate)
    return jnp.minimum(chosen, 0.9).astype(jnp.float32)


def level_of(rng, extent, shards, low, largest):
    factor_of = 1.0
    for axis_at, blocks in shards:
        heights = jax.random.uniform(jax.random.fold_in(jax.random.fold_in(rng, 6), axis_at), (blocks,), jnp.float32, low / len(shards), largest / len(shards))
        factor_of = factor_of * jnp.repeat(jnp.exp(heights), extent[axis_at] // blocks).reshape((-1,) + (1,) * (len(extent) - 1 - axis_at))
    return factor_of


def gaussian(own_key, shape, spread, bound, shards=(), held_as=jnp.bfloat16):
    drawn = jax.random.normal(own_key, shape, jnp.float32) * spread
    if len(shards) > 0:
        drawn = level_of(own_key, shape, shards, -0.22, 0.18) * drawn
    return jnp.clip(drawn, min=-bound, max=bound).astype(held_as)


def setup_inputs(seed: int = 0) -> dict:
    key_of = jax.random.split(jax.random.key(seed), 12)
    return {
        "layer_in": gaussian(key_of[0], (SEQLEN, D), 1.0, 6.0, ((0, 8), (1, 4))),
        "attn_gain": jnp.clip(1.0 + 0.18 * jax.random.normal(key_of[1], (D,), jnp.float32), 0.1, 1.9),
        "qkv_weight": gaussian(key_of[2], (3, D, HEADS * DK), D ** -0.5, 0.125, ((2, 4),)),
        "log_decay": draw_log_decay(jax.random.fold_in(key_of[11], 71), 0),
        "write_rate": draw_write_rate(jax.random.fold_in(key_of[11], 71), 0),
        "head_gain": jnp.clip(1.0 + 0.18 * jax.random.normal(key_of[5], (DK,), jnp.float32), 0.1, 1.9),
        "out_weight": gaussian(key_of[6], (HEADS * DK, D), (HEADS * DK) ** -0.5, 0.1875, ((0, 4),)),
        "ffn_gain": jnp.clip(1.0 + 0.18 * jax.random.normal(key_of[7], (D,), jnp.float32), 0.1, 1.9),
        "gate_weight": gaussian(key_of[8], (D, FF), D ** -0.5, 0.125, ((1, 4),)),
        "up_weight": gaussian(key_of[9], (D, FF), D ** -0.5, 0.125, ((1, 4),)),
        "down_weight": gaussian(key_of[10], (FF, D), FF ** -0.5, 0.125, ((0, 4),)),
    }


norm_floor = 0.1
head_floor = 0.05

def rms_scale(values, gain, floor):
    return values * lax.rsqrt(lax.optimization_barrier(jnp.mean(values * values, axis=-1, keepdims=True)) + floor) * gain

def unit_rows(vectors):
    return vectors * lax.rsqrt(lax.optimization_barrier(jnp.sum(vectors * vectors, axis=-1, keepdims=True)) + 1.0)

def grouped_sum(left_side, right_side, groups):
    group_span = right_side.shape[0] // groups
    running = jnp.zeros((left_side.shape[0], right_side.shape[1]), jnp.float32)
    for member in range(groups):
        partial_value = jnp.dot(left_side[:, member * group_span:(member + 1) * group_span], right_side[member * group_span:(member + 1) * group_span], preferred_element_type=jnp.float32)
        running = running + partial_value.astype(jnp.bfloat16).astype(jnp.float32)
    return running

def token_step(memory, inputs):
    queries, key_rows, values, decay_step, write_step = inputs
    projected = lax.optimization_barrier(jnp.sum(key_rows[:, :, None] * memory, axis=1))
    memory = decay_step[:, None, None] * (memory - write_step[:, None, None] * key_rows[:, :, None] * projected[:, None, :]) + write_step[:, None, None] * key_rows[:, :, None] * values[:, None, :]
    output = lax.optimization_barrier(jnp.sum(queries[:, :, None] * memory, axis=1))
    return (memory, output)

def reference(layer_in, attn_gain, qkv_weight, log_decay, write_rate, head_gain, out_weight, ffn_gain, gate_weight, up_weight, down_weight):
    inputs = layer_in.astype(jnp.float32)
    normed = rms_scale(inputs, attn_gain, norm_floor).astype(jnp.bfloat16)
    queries = jnp.dot(normed, qkv_weight[0], preferred_element_type=jnp.float32).reshape(SEQLEN, HEADS, DK)
    key_rows = jnp.dot(normed, qkv_weight[1], preferred_element_type=jnp.float32).reshape(SEQLEN, HEADS, DK)
    values = jnp.dot(normed, qkv_weight[2], preferred_element_type=jnp.float32).reshape(SEQLEN, HEADS, DK)
    queries = unit_rows(queries)
    key_rows = unit_rows(key_rows)
    start = jnp.zeros((HEADS, DK, DK), jnp.float32)
    final_memory, heads_raw = lax.scan(token_step, start, (queries, key_rows, values, jnp.exp(log_decay).T, write_rate.T))
    heads_out = rms_scale(heads_raw, head_gain, head_floor).reshape(SEQLEN, HEADS * DK).astype(jnp.bfloat16)
    attn = grouped_sum(heads_out, out_weight, N_TP)
    residual = inputs + attn
    normed_mid = rms_scale(residual, ffn_gain, norm_floor).astype(jnp.bfloat16)
    gate_act = jnp.dot(normed_mid, gate_weight, preferred_element_type=jnp.float32)
    up_act = jnp.dot(normed_mid, up_weight, preferred_element_type=jnp.float32)
    hidden = (jax.nn.silu(gate_act) * up_act).astype(jnp.bfloat16)
    ffn = grouped_sum(hidden, down_weight, N_TP)
    return (residual + ffn).astype(jnp.bfloat16)
```

```python
import functools

import jax
import jax.numpy as jnp
from jax import lax
from jax.experimental import pallas as pl
from jax.experimental.pallas import tpu as pltpu
from jax.sharding import PartitionSpec as P

norm_floor = 0.1
head_floor = 0.05
parts_of_block = 2
radix = 3
f32 = jnp.float32
bf16 = jnp.bfloat16
vmem = pl.BlockSpec(memory_space=pltpu.VMEM)
smem = pl.BlockSpec(memory_space=pltpu.SMEM)
roomy = pltpu.CompilerParams(vmem_limit_bytes=56 * 1024 * 1024)


def mm(a, b):
    return jnp.dot(a.astype(bf16), b.astype(bf16), preferred_element_type=f32)


def mm_nt(a, b):
    return lax.dot_general(
        a.astype(bf16), b.astype(bf16), (((1,), (1,)), ((), ())), preferred_element_type=f32
    )


def mm_tn(a, b):
    return lax.dot_general(
        a.astype(bf16), b.astype(bf16), (((0,), (0,)), ((), ())), preferred_element_type=f32
    )


def halves(a):
    high = a.astype(bf16)
    return high, (a - high.astype(f32)).astype(bf16)


def mm_split(a, b):
    a_high, a_low = a
    b_high, b_low = b
    return mm(a_high, b_high) + (mm(a_high, b_low) + mm(a_low, b_high))


def swap(x, axis, bit):
    peers = lax.axis_size(axis)
    return lax.ppermute(x, axis, [(i, i ^ bit) for i in range(peers)])


def gather_pieces(x, axis):
    bit = lax.axis_size(axis) // 2
    pieces = {0: x}
    while bit:
        pieces.update({r | bit: swap(piece, axis, bit) for r, piece in pieces.items()})
        bit //= 2
    return [pieces[r] for r in range(len(pieces))]


def scatter_pieces(pieces, axis):
    peers = lax.axis_size(axis)
    bit = 1
    while bit < peers:
        keep = [r for r in pieces if not r & bit]
        moved = {r: swap(pieces[r | bit].astype(bf16), axis, bit).astype(f32) for r in keep}
        pieces = {r: pieces[r].astype(f32) + moved[r] for r in keep}
        bit *= 2
    return pieces[0]


def unit(rows):
    return rows * lax.rsqrt(jnp.sum(rows * rows, axis=1, keepdims=True) + 1.0)


def front_kernel(*refs, peers, heads, span):
    me_ref = refs[0]
    piece_refs = refs[1 : 1 + peers]
    gain_ref, weight_ref, cumul_ref, rate_ref = refs[1 + peers : 5 + peers]
    whole_ref, local_ref, entry_ref, map_ref, proj_ref = refs[5 + peers :]
    me = me_ref[0]
    length, slice_width = piece_refs[0].shape
    width = map_ref.shape[1]
    pieces = length // span
    for r in range(peers):
        at = pl.multiple_of((me ^ r) * slice_width, slice_width)
        whole_ref[:, pl.ds(at, slice_width)] = piece_refs[r][...]
    for c in range(pieces):
        rows = whole_ref[c * span : (c + 1) * span, :].astype(f32)
        normed = (
            rows
            * lax.rsqrt(jnp.mean(rows * rows, axis=1, keepdims=True) + norm_floor)
            * gain_ref[...]
        ).astype(bf16)
        for kind in range(3):
            proj_ref[kind, c * span : (c + 1) * span, :] = jnp.dot(
                normed, weight_ref[kind], preferred_element_type=f32
            )
    row_ids = lax.broadcasted_iota(jnp.int32, (span, span), 0)
    col_ids = lax.broadcasted_iota(jnp.int32, (span, span), 1)
    eye = (row_ids == col_ids).astype(f32)
    units = [(h, c) for h in range(heads) for c in range(pieces)]

    def operands(h, c):
        at = (slice(c * span, (c + 1) * span), slice(h * width, (h + 1) * width))
        cumul_row = jnp.broadcast_to(cumul_ref[h, c : c + 1, :], (span, span))
        rate = jnp.broadcast_to(rate_ref[h, c : c + 1, :], (span, span)).T
        cumul = cumul_row.T
        decay = jnp.where(
            row_ids >= col_ids, jnp.exp(jnp.minimum(cumul - cumul_row, 0.0)), 0.0
        )
        return at, cumul, cumul_row, rate, decay

    lowers = []
    inverses = []
    for h, c in units:
        at, cumul, cumul_row, rate, decay = operands(h, c)
        keys = unit(proj_ref[(1,) + at])
        proj_ref[(1,) + at] = keys
        lower = jnp.where(row_ids > col_ids, rate * mm_nt(keys, keys) * decay, 0.0)
        lowers.append(lower)
        inverses.append(eye - jnp.where(row_ids >> 1 == col_ids >> 1, lower, 0.0))
    level = 1
    while (1 << level) < span:
        joins = (row_ids >> (level + 1) == col_ids >> (level + 1)) & (
            row_ids >> level != col_ids >> level
        )
        for u in range(len(units)):
            split = halves(inverses[u])
            inner = mm_split(halves(jnp.where(joins, lowers[u], 0.0)), split)
            inverses[u] = inverses[u] - mm_split(split, halves(inner))
        level += 1
    for h in range(heads):
        carried = jnp.concatenate(
            [
                (
                    lax.broadcasted_iota(jnp.int32, (width, width), 0)
                    == lax.broadcasted_iota(jnp.int32, (width, width), 1)
                ).astype(f32),
                jnp.zeros((width, width), f32),
            ],
            axis=1,
        )
        for c in range(pieces):
            at, cumul, cumul_row, rate, decay = operands(h, c)
            keys = proj_ref[(1,) + at]
            queries = unit(proj_ref[(0,) + at])
            rate_col = rate[:, :1]
            growth = jnp.exp(cumul[:, :1])
            last = cumul_row[:1, span - 1 :]
            right_side = jnp.concatenate(
                [rate_col * growth * keys, rate_col * proj_ref[(2,) + at]], axis=1
            )
            solved = mm(inverses[h * pieces + c], right_side)
            mixed = mm(mm_nt(queries, keys) * decay, solved)
            tail = mm_tn(keys * jnp.exp(last - cumul[:, :1]), solved)
            entry = growth * queries - mixed[:, :width]
            reached = mm(entry, carried)
            rows_at = slice(c * span, (c + 1) * span)
            entry_ref[h, rows_at, :] = reached[:, :width].astype(bf16)
            local_ref[h, rows_at, :] = reached[:, width:] + mixed[:, width:]
            change = mm(tail[:, :width], carried)
            carried = jnp.exp(last) * carried - change
            carried = jnp.concatenate(
                [carried[:, :width], carried[:, width:] + tail[:, width:]], axis=1
            )
        map_ref[h] = carried.astype(bf16)


def joined(maps, h, width):
    acc = maps[-1][h].astype(f32)
    for one in reversed(maps[:-1]):
        acc = mm(one[h, :, :width], acc)
        shift = one[h, :, width:].astype(f32)
        if acc.shape[1] == width:
            acc = acc + shift
        else:
            acc = jnp.concatenate([acc[:, :width], acc[:, width:] + shift], axis=1)
    return acc


def join_kernel(*refs):
    out_ref = refs[-1]
    width = out_ref.shape[1]
    for h in range(out_ref.shape[0]):
        out_ref[h] = joined(refs[:-1], h, width).astype(bf16)


def heads_kernel(*refs, count):
    map_refs = refs[:count]
    local_ref, entry_ref, gain_ref = refs[count : count + 3]
    out_refs = refs[count + 3 :]
    heads, length, width = local_ref.shape
    rows = length // len(out_refs)
    for h in range(heads):
        state = joined(map_refs, h, width)
        if state.shape[1] != width:
            state = state[:, width:]
        for part, out_ref in enumerate(out_refs):
            at = slice(part * rows, (part + 1) * rows)
            raw = local_ref[h, at, :] + mm(entry_ref[h, at, :], state)
            out_ref[:, h * width : (h + 1) * width] = (
                raw
                * lax.rsqrt(jnp.mean(raw * raw, axis=1, keepdims=True) + head_floor)
                * gain_ref[...]
            ).astype(bf16)


def back_kernel(*refs, peers):
    me_ref = refs[0]
    head_refs = refs[1 : 1 + peers]
    out_weight_refs = refs[1 + peers : 1 + 2 * peers]
    whole_ref, gain_ref, gate_ref, up_ref, down_ref = refs[1 + 2 * peers : 6 + 2 * peers]
    own_ref = refs[6 + 2 * peers]
    term_refs = refs[7 + 2 * peers : 7 + 3 * peers]
    residual_ref = refs[-1]
    me = me_ref[0]
    slice_width = own_ref.shape[1]
    attn = jnp.dot(head_refs[0][...], out_weight_refs[0][...], preferred_element_type=f32)
    for r in range(1, peers):
        attn = attn + jnp.dot(
            head_refs[r][...], out_weight_refs[r][...], preferred_element_type=f32
        )
    residual = whole_ref[...].astype(f32) + attn
    residual_ref[...] = residual
    normed = (
        residual
        * lax.rsqrt(jnp.mean(residual * residual, axis=1, keepdims=True) + norm_floor)
        * gain_ref[...]
    ).astype(bf16)
    gate = jnp.dot(normed, gate_ref[...], preferred_element_type=f32)
    up = jnp.dot(normed, up_ref[...], preferred_element_type=f32)
    hidden = (jax.nn.silu(gate) * up).astype(bf16)
    for r in reversed(range(peers)):
        at = pl.multiple_of((me ^ r) * slice_width, slice_width)
        term_refs[r][...] = jnp.dot(
            hidden, down_ref[:, pl.ds(at, slice_width)], preferred_element_type=f32
        ).astype(bf16)
    at = pl.multiple_of(me * slice_width, slice_width)
    own_ref[...] = residual_ref[:, pl.ds(at, slice_width)]


def call(kernel, outs, args, scratch=(), first_smem=True):
    return pl.pallas_call(
        kernel,
        out_shape=[jax.ShapeDtypeStruct(s, d) for s, d in outs],
        in_specs=[smem if first_smem and i == 0 else vmem for i in range(len(args))],
        out_specs=[vmem] * len(outs),
        scratch_shapes=list(scratch),
        compiler_params=roomy,
    )(*args)


def shifted(x, axis, by):
    peers = lax.axis_size(axis)
    return lax.ppermute(x, axis, [(i, i + by) for i in range(peers - by)])


def earlier_maps(maps, axis):
    peers = lax.axis_size(axis)
    width = maps.shape[1]
    window = 1
    while window * radix < peers - 1:
        terms = [maps] + [shifted(maps, axis, window * k) for k in range(1, radix)]
        maps = call(join_kernel, [(maps.shape, bf16)], terms, first_smem=False)[0]
        window *= radix
    offsets = list(range(1, peers, window))
    moved = [shifted(maps, axis, by) for by in offsets[:-1]]
    return moved + [shifted(maps[:, :, width:], axis, by) for by in offsets[-1:]]


def body(
    layer_in,
    attn_gain,
    qkv_weight,
    log_decay,
    write_rate,
    head_gain,
    out_weight,
    ffn_gain,
    gate_weight,
    up_weight,
    down_weight,
):
    length, slice_width = layer_in.shape
    width = head_gain.shape[0]
    local_heads = qkv_weight.shape[2] // width
    model = attn_gain.shape[0]
    peers = lax.axis_size("tp")
    me = lax.axis_index("tp").astype(jnp.int32).reshape(1)
    span = min(128, length)
    count = length // span
    pieces = gather_pieces(layer_in, "tp")
    cumul = jnp.cumsum(log_decay.reshape(local_heads, count, span), axis=2)
    held = lax.optimization_barrier((out_weight, pieces[peers // 2]))
    weight_pieces = gather_pieces(held[0], "tp")
    whole, local, entry, maps = call(
        functools.partial(front_kernel, peers=peers, heads=local_heads, span=span),
        [
            ((length, model), bf16),
            ((local_heads, length, width), f32),
            ((local_heads, length, width), bf16),
            ((local_heads, width, 2 * width), bf16),
        ],
        [
            me,
            *pieces,
            attn_gain.reshape(1, model),
            qkv_weight,
            cumul,
            write_rate.reshape(local_heads, count, span),
        ],
        scratch=[pltpu.VMEM((3, length, local_heads * width), f32)],
    )
    before = earlier_maps(maps, "seq")
    rows = length // parts_of_block
    heads_out = call(
        functools.partial(heads_kernel, count=len(before)),
        [((rows, local_heads * width), bf16)] * parts_of_block,
        [*before, local, entry, head_gain.reshape(1, width)],
        first_smem=False,
    )
    results = []
    gathered = [gather_pieces(part, "tp") for part in heads_out]
    for part in range(parts_of_block):
        own, *terms = call(
            functools.partial(back_kernel, peers=peers),
            [((rows, slice_width), f32)] + [((rows, slice_width), bf16)] * peers,
            [
                me,
                *gathered[part],
                *weight_pieces,
                lax.slice_in_dim(whole, part * rows, (part + 1) * rows),
                ffn_gain.reshape(1, model),
                gate_weight,
                up_weight,
                down_weight,
            ],
            scratch=[pltpu.VMEM((rows, model), f32)],
        )
        shared = scatter_pieces(dict(enumerate(terms)), "tp")
        results.append((own + shared).astype(bf16))
    return jnp.concatenate(results, axis=0)


def solution(mesh):
    placed = (
        P("seq", "tp"),
        P(),
        P(None, None, "tp"),
        P("tp", "seq"),
        P("tp", "seq"),
        P(),
        P("tp", None),
        P(),
        P(None, "tp"),
        P(None, "tp"),
        P("tp", None),
    )
    return jax.shard_map(
        body, mesh=mesh, in_specs=placed, out_specs=P("seq", "tp"), check_vma=False
    )
```

```python
import functools

import jax
import jax.numpy as jnp
from jax import lax
from jax.experimental import pallas as pl
from jax.experimental.pallas import tpu as pltpu
from jax.sharding import PartitionSpec as P


norm_floor = 0.1
head_floor = 0.05
parts_of_block = 2
radix = 3
f32 = jnp.float32
bf16 = jnp.bfloat16
vmem = pl.BlockSpec(memory_space=pltpu.VMEM)
smem = pl.BlockSpec(memory_space=pltpu.SMEM)
mebi = 1024 * 1024


def mm(a, b):
    return jnp.dot(a.astype(bf16), b.astype(bf16), preferred_element_type=f32)


def mm_nt(a, b):
    return lax.dot_general(
        a.astype(bf16), b.astype(bf16), (((1,), (1,)), ((), ())), preferred_element_type=f32
    )


def mm_tn(a, b):
    return lax.dot_general(
        a.astype(bf16), b.astype(bf16), (((0,), (0,)), ((), ())), preferred_element_type=f32
    )


def halves(a):
    high = a.astype(bf16)
    return high, (a - high.astype(f32)).astype(bf16)


def mm_split(a, b):
    a_high, a_low = a
    b_high, b_low = b
    return mm(a_high, b_high) + (mm(a_high, b_low) + mm(a_low, b_high))


def swap(x, axis, bit):
    peers = lax.axis_size(axis)
    return lax.ppermute(x, axis, [(i, i ^ bit) for i in range(peers)])


def gather_pieces(x, axis, far=None):
    bit = lax.axis_size(axis) // 2
    pieces = {0: x}
    if far is not None:
        pieces[bit] = far
        bit //= 2
    while bit:
        pieces.update({r | bit: swap(piece, axis, bit) for r, piece in pieces.items()})
        bit //= 2
    return [pieces[r] for r in range(len(pieces))]


def scatter_step(pieces, axis, bit):
    keep = [r for r in pieces if not r & bit]
    moved = {r: swap(pieces[r | bit].astype(bf16), axis, bit).astype(f32) for r in keep}
    return {r: pieces[r].astype(f32) + moved[r] for r in keep}


def scatter_near(pieces, axis):
    bit = 1
    while bit < lax.axis_size(axis) // 2:
        pieces = scatter_step(pieces, axis, bit)
        bit *= 2
    return {r: piece.astype(bf16) if r & bit else piece for r, piece in pieces.items()}


def scatter_far(pieces, axis):
    return scatter_step(pieces, axis, lax.axis_size(axis) // 2)[0]


def unit(rows):
    return rows * lax.rsqrt(jnp.sum(rows * rows, axis=1, keepdims=True) + 1.0)


def front_kernel(*refs, peers, heads, span, part, first):
    me_ref = refs[0]
    piece_refs = refs[1 : 1 + peers]
    gain_ref, weight_ref, log_ref, rate_ref = refs[1 + peers : 5 + peers]
    carry_refs = () if first else refs[5 + peers : 6 + peers]
    whole_ref, local_ref, entry_ref, map_ref, proj_ref = refs[5 + peers + len(carry_refs) :]
    me = me_ref[0]
    length, slice_width = piece_refs[0].shape
    width = map_ref.shape[1]
    pieces = length // span
    for r in range(peers):
        at = pl.multiple_of((me ^ r) * slice_width, slice_width)
        whole_ref[:, pl.ds(at, slice_width)] = piece_refs[r][...]
    for c in range(pieces):
        rows = whole_ref[c * span : (c + 1) * span, :].astype(f32)
        normed = (
            rows
            * lax.rsqrt(jnp.mean(rows * rows, axis=1, keepdims=True) + norm_floor)
            * gain_ref[...]
        ).astype(bf16)
        for kind in range(3):
            proj_ref[kind, c * span : (c + 1) * span, :] = jnp.dot(
                normed, weight_ref[kind], preferred_element_type=f32
            )
    row_ids = lax.broadcasted_iota(jnp.int32, (span, span), 0)
    col_ids = lax.broadcasted_iota(jnp.int32, (span, span), 1)
    eye = (row_ids == col_ids).astype(f32)
    units = [(h, c) for h in range(heads) for c in range(pieces)]
    begin = part * length
    cumul_rows = jnp.dot(
        jnp.concatenate(
            [log_ref[h : h + 1, begin + c * span : begin + (c + 1) * span] for h, c in units]
        ),
        (row_ids <= col_ids).astype(f32),
        precision=lax.Precision.HIGHEST,
        preferred_element_type=f32,
    )

    def operands(h, c):
        at = (slice(c * span, (c + 1) * span), slice(h * width, (h + 1) * width))
        u = h * pieces + c
        cumul_row = jnp.broadcast_to(cumul_rows[u : u + 1, :], (span, span))
        rate = jnp.broadcast_to(
            rate_ref[h : h + 1, begin + c * span : begin + (c + 1) * span], (span, span)
        ).T
        cumul = cumul_row.T
        decay = jnp.where(
            row_ids >= col_ids, jnp.exp(jnp.minimum(cumul - cumul_row, 0.0)), 0.0
        )
        return at, cumul, cumul_row, rate, decay

    lowers = []
    inverses = []
    for h, c in units:
        at, cumul, cumul_row, rate, decay = operands(h, c)
        keys = unit(proj_ref[(1,) + at])
        proj_ref[(1,) + at] = keys
        lower = jnp.where(row_ids > col_ids, rate * mm_nt(keys, keys) * decay, 0.0)
        lowers.append(lower)
        inverses.append(eye - jnp.where(row_ids >> 1 == col_ids >> 1, lower, 0.0))
    level = 1
    while (1 << level) < span:
        joins = (row_ids >> (level + 1) == col_ids >> (level + 1)) & (
            row_ids >> level != col_ids >> level
        )
        for u in range(len(units)):
            split = halves(inverses[u])
            inner = mm_split(halves(jnp.where(joins, lowers[u], 0.0)), split)
            inverses[u] = inverses[u] - mm_split(split, halves(inner))
        level += 1
    for h in range(heads):
        if first:
            carried = (
                lax.broadcasted_iota(jnp.int32, (width, 2 * width), 0)
                == lax.broadcasted_iota(jnp.int32, (width, 2 * width), 1)
            ).astype(f32)
        else:
            carried = carry_refs[0][h]
        for c in range(pieces):
            at, cumul, cumul_row, rate, decay = operands(h, c)
            keys = proj_ref[(1,) + at]
            queries = unit(proj_ref[(0,) + at])
            rate_col = rate[:, :1]
            growth = jnp.exp(cumul[:, :1])
            last = cumul_row[:1, span - 1 :]
            right_side = jnp.concatenate(
                [rate_col * growth * keys, rate_col * proj_ref[(2,) + at]], axis=1
            )
            solved = mm(inverses[h * pieces + c], right_side)
            mixed = mm(mm_nt(queries, keys) * decay, solved)
            tail = mm_tn(keys * jnp.exp(last - cumul[:, :1]), solved)
            entry = growth * queries - mixed[:, :width]
            reached = mm(entry, carried)
            rows_at = slice(c * span, (c + 1) * span)
            entry_ref[h, rows_at, :] = reached[:, :width].astype(bf16)
            local_ref[h, rows_at, :] = reached[:, width:] + mixed[:, width:]
            change = mm(tail[:, :width], carried)
            carried = jnp.exp(last) * carried - change
            carried = jnp.concatenate(
                [carried[:, :width], carried[:, width:] + tail[:, width:]], axis=1
            )
        map_ref[h] = carried.astype(map_ref.dtype)


def joined(maps, h, width):
    acc = maps[-1][h].astype(f32)
    for one in reversed(maps[:-1]):
        acc = mm(one[h, :, :width], acc)
        shift = one[h, :, width:].astype(f32)
        if acc.shape[1] == width:
            acc = acc + shift
        else:
            acc = jnp.concatenate([acc[:, :width], acc[:, width:] + shift], axis=1)
    return acc


def join_kernel(*refs):
    out_ref, shift_ref = refs[-2:]
    width = out_ref.shape[1]
    for h in range(out_ref.shape[0]):
        acc = joined(refs[:-2], h, width).astype(bf16)
        out_ref[h] = acc
        shift_ref[h] = acc[:, width:]


def heads_kernel(*refs, count, parts):
    map_refs = refs[:count]
    local_refs = refs[count : count + parts]
    entry_refs = refs[count + parts : count + 2 * parts]
    gain_ref = refs[count + 2 * parts]
    out_refs = refs[count + 2 * parts + 1 :]
    heads, _, width = local_refs[0].shape
    for h in range(heads):
        state = joined(map_refs, h, width)
        if state.shape[1] != width:
            state = state[:, width:]
        for part, out_ref in enumerate(out_refs):
            raw = local_refs[part][h] + mm(entry_refs[part][h], state)
            out_ref[:, h * width : (h + 1) * width] = (
                raw
                * lax.rsqrt(jnp.mean(raw * raw, axis=1, keepdims=True) + head_floor)
                * gain_ref[...]
            ).astype(bf16)


def back_kernel(*refs, peers):
    me_ref = refs[0]
    head_refs = refs[1 : 1 + peers]
    out_weight_refs = refs[1 + peers : 1 + 2 * peers]
    whole_ref, gain_ref, gate_ref, up_ref, down_ref = refs[1 + 2 * peers : 6 + 2 * peers]
    own_ref = refs[6 + 2 * peers]
    term_refs = refs[7 + 2 * peers : 7 + 3 * peers]
    residual_ref = refs[-1]
    me = me_ref[0]
    slice_width = own_ref.shape[1]
    attn = jnp.dot(head_refs[0][...], out_weight_refs[0][...], preferred_element_type=f32)
    for r in range(1, peers):
        attn = attn + jnp.dot(
            head_refs[r][...], out_weight_refs[r][...], preferred_element_type=f32
        )
    residual = whole_ref[...].astype(f32) + attn
    residual_ref[...] = residual
    normed = (
        residual
        * lax.rsqrt(jnp.mean(residual * residual, axis=1, keepdims=True) + norm_floor)
        * gain_ref[...]
    ).astype(bf16)
    gate = jnp.dot(normed, gate_ref[...], preferred_element_type=f32)
    up = jnp.dot(normed, up_ref[...], preferred_element_type=f32)
    hidden = (jax.nn.silu(gate) * up).astype(bf16)
    for r in reversed(range(peers)):
        at = pl.multiple_of((me ^ r) * slice_width, slice_width)
        term_refs[r][...] = jnp.dot(
            hidden, down_ref[:, pl.ds(at, slice_width)], preferred_element_type=f32
        ).astype(bf16)
    at = pl.multiple_of(me * slice_width, slice_width)
    own_ref[...] = residual_ref[:, pl.ds(at, slice_width)]


def call(kernel, outs, args, scratch=(), first_smem=True, flops=10**9, room=8):
    return pl.pallas_call(
        kernel,
        out_shape=[jax.ShapeDtypeStruct(s, d) for s, d in outs],
        in_specs=[smem if first_smem and i == 0 else vmem for i in range(len(args))],
        out_specs=[vmem] * len(outs),
        scratch_shapes=list(scratch),
        compiler_params=pltpu.CompilerParams(vmem_limit_bytes=room * mebi),
        cost_estimate=pl.CostEstimate(flops=flops, bytes_accessed=0, transcendentals=0),
    )(*args)


def shifted(x, axis, by):
    peers = lax.axis_size(axis)
    return lax.ppermute(x, axis, [(i, i + by) for i in range(peers - by)])


def earlier_maps(maps, axis):
    peers = lax.axis_size(axis)
    width = maps.shape[1]
    window = 1
    shift = None
    while window * radix < peers - 1:
        terms = [maps] + [shifted(maps, axis, window * k) for k in range(1, radix)]
        maps, shift = call(
            join_kernel,
            [(maps.shape, bf16), (maps.shape[:2] + (width,), bf16)],
            terms,
            first_smem=False,
        )
        window *= radix
    if shift is None:
        shift = maps[:, :, width:]
    offsets = list(range(1, peers, window))
    moved = [shifted(maps, axis, by) for by in offsets[:-1]]
    return moved + [shifted(shift, axis, by) for by in offsets[-1:]]


def body(
    layer_in,
    attn_gain,
    qkv_weight,
    log_decay,
    write_rate,
    head_gain,
    out_weight,
    ffn_gain,
    gate_weight,
    up_weight,
    down_weight,
):
    length, slice_width = layer_in.shape
    width = head_gain.shape[0]
    local_heads = qkv_weight.shape[2] // width
    model = attn_gain.shape[0]
    peers = lax.axis_size("tp")
    me = lax.axis_index("tp").astype(jnp.int32).reshape(1)
    parts = parts_of_block
    rows = length // parts
    span = min(128, rows)
    pieces = [
        gather_pieces(lax.slice_in_dim(layer_in, part * rows, (part + 1) * rows), "tp")
        for part in range(parts)
    ]
    held = lax.optimization_barrier((out_weight, pieces[-1][peers // 2]))[0]
    weight_far = swap(held, "tp", peers // 2)
    wholes, locals_, entries = [], [], []
    carried = ()
    for part in range(parts):
        last = part == parts - 1
        whole, local, entry, maps = call(
            functools.partial(
                front_kernel,
                peers=peers,
                heads=local_heads,
                span=span,
                part=part,
                first=part == 0,
            ),
            [
                ((rows, model), bf16),
                ((local_heads, rows, width), f32),
                ((local_heads, rows, width), bf16),
                ((local_heads, width, 2 * width), bf16 if last else f32),
            ],
            [
                me,
                *pieces[part],
                attn_gain.reshape(1, model),
                qkv_weight,
                log_decay,
                write_rate,
                *carried,
            ],
            scratch=[pltpu.VMEM((3, rows, local_heads * width), f32)],
            flops=8 * 10**9,
            room=20,
        )
        carried = (maps,)
        wholes.append(whole)
        locals_.append(local)
        entries.append(entry)
    before = earlier_maps(maps, "seq")
    heads_out = call(
        functools.partial(heads_kernel, count=len(before), parts=parts),
        [((rows, local_heads * width), bf16)] * parts,
        [*before, *locals_, *entries, head_gain.reshape(1, width)],
        first_smem=False,
        flops=3 * 10**9,
    )
    weight_far, out_held, *heads_out = lax.optimization_barrier(
        (weight_far, out_weight, *heads_out)
    )
    weight_pieces = gather_pieces(out_held, "tp", weight_far)
    results = []
    gathered = []
    for shard in heads_out:
        lead = swap
        gathered.append(gather_pieces(shard, "tp", lead(shard, "tp", peers // 2)))
    for part in range(parts):
        back = call
        far = scatter_far
        own, *terms = back(
            functools.partial(back_kernel, peers=peers),
            [((rows, slice_width), f32)] + [((rows, slice_width), bf16)] * peers,
            [
                me,
                *gathered[part],
                *weight_pieces,
                wholes[part],
                ffn_gain.reshape(1, model),
                gate_weight,
                up_weight,
                down_weight,
            ],
            scratch=[pltpu.VMEM((rows, model), f32)],
            flops=6 * 10**9,
            room=28,
        )
        terms = scatter_near(dict(enumerate(terms)), "tp")
        if part + 1 < parts:
            gathered[part + 1], terms = lax.optimization_barrier((gathered[part + 1], terms))
        shared = far(terms, "tp")
        results.append((own + shared).astype(bf16))
    return jnp.concatenate(results, axis=0)


def solution(mesh):
    placed = (
        P("seq", "tp"),
        P(),
        P(None, None, "tp"),
        P("tp", "seq"),
        P("tp", "seq"),
        P(),
        P("tp", None),
        P(),
        P(None, "tp"),
        P(None, "tp"),
        P("tp", None),
    )
    return jax.shard_map(
        body, mesh=mesh, in_specs=placed, out_specs=P("seq", "tp"), check_vma=False
    )
```

```python
import functools

import jax
import jax.numpy as jnp
from jax import lax
from jax.experimental import pallas as pl
from jax.experimental.pallas import tpu as pltpu
from jax.sharding import PartitionSpec as P


norm_floor = 0.1
head_floor = 0.05
parts_of_block = 3
radix = 3
f32 = jnp.float32
bf16 = jnp.bfloat16
vmem = pl.BlockSpec(memory_space=pltpu.VMEM)
smem = pl.BlockSpec(memory_space=pltpu.SMEM)
mebi = 1024 * 1024


def mm(a, b):
    return jnp.dot(a.astype(bf16), b.astype(bf16), preferred_element_type=f32)


def mm_nt(a, b):
    return lax.dot_general(
        a.astype(bf16), b.astype(bf16), (((1,), (1,)), ((), ())), preferred_element_type=f32
    )


def mm_tn(a, b):
    return lax.dot_general(
        a.astype(bf16), b.astype(bf16), (((0,), (0,)), ((), ())), preferred_element_type=f32
    )


def halves(a):
    high = a.astype(bf16)
    return high, (a - high.astype(f32)).astype(bf16)


def mm_split(a, b):
    a_high, a_low = a
    b_high, b_low = b
    return mm(a_high, b_high) + (mm(a_high, b_low) + mm(a_low, b_high))


def swap(x, axis, bit):
    peers = lax.axis_size(axis)
    return lax.ppermute(x, axis, [(i, i ^ bit) for i in range(peers)])


def gather_pieces(x, axis, far=None):
    bit = lax.axis_size(axis) // 2
    pieces = {0: x}
    if far is not None:
        pieces[bit] = far
        bit //= 2
    while bit:
        pieces.update({r | bit: swap(piece, axis, bit) for r, piece in pieces.items()})
        bit //= 2
    return [pieces[r] for r in range(len(pieces))]


def scatter_step(pieces, axis, bit):
    keep = [r for r in pieces if not r & bit]
    moved = {r: swap(pieces[r | bit].astype(bf16), axis, bit).astype(f32) for r in keep}
    return {r: pieces[r].astype(f32) + moved[r] for r in keep}


def scatter_near(pieces, axis):
    bit = 1
    while bit < lax.axis_size(axis) // 2:
        pieces = scatter_step(pieces, axis, bit)
        bit *= 2
    return {r: piece.astype(bf16) if r & bit else piece for r, piece in pieces.items()}


def scatter_far(pieces, axis):
    return scatter_step(pieces, axis, lax.axis_size(axis) // 2)[0]


def unit(rows):
    return rows * lax.rsqrt(jnp.sum(rows * rows, axis=1, keepdims=True) + 1.0)


def front_kernel(*refs, peers, heads, span, part, first):
    me_ref = refs[0]
    piece_refs = refs[1 : 1 + peers]
    gain_ref, weight_ref, log_ref, rate_ref = refs[1 + peers : 5 + peers]
    carry_refs = () if first else refs[5 + peers : 6 + peers]
    whole_ref, local_ref, entry_ref, map_ref, proj_ref = refs[5 + peers + len(carry_refs) :]
    me = me_ref[0]
    length, slice_width = piece_refs[0].shape
    width = map_ref.shape[1]
    pieces = length // span
    for r in range(peers):
        at = pl.multiple_of((me ^ r) * slice_width, slice_width)
        whole_ref[:, pl.ds(at, slice_width)] = piece_refs[r][...]
    for c in range(pieces):
        rows = whole_ref[c * span : (c + 1) * span, :].astype(f32)
        normed = (
            rows
            * lax.rsqrt(jnp.mean(rows * rows, axis=1, keepdims=True) + norm_floor)
            * gain_ref[...]
        ).astype(bf16)
        for kind in range(3):
            proj_ref[kind, c * span : (c + 1) * span, :] = jnp.dot(
                normed, weight_ref[kind], preferred_element_type=f32
            )
    row_ids = lax.broadcasted_iota(jnp.int32, (span, span), 0)
    col_ids = lax.broadcasted_iota(jnp.int32, (span, span), 1)
    eye = (row_ids == col_ids).astype(f32)
    units = [(h, c) for h in range(heads) for c in range(pieces)]
    begin = part * length
    cumul_rows = jnp.dot(
        jnp.concatenate(
            [log_ref[h : h + 1, begin + c * span : begin + (c + 1) * span] for h, c in units]
        ),
        (row_ids <= col_ids).astype(f32),
        precision=lax.Precision.HIGHEST,
        preferred_element_type=f32,
    )

    def operands(h, c):
        at = (slice(c * span, (c + 1) * span), slice(h * width, (h + 1) * width))
        u = h * pieces + c
        cumul_row = jnp.broadcast_to(cumul_rows[u : u + 1, :], (span, span))
        rate = jnp.broadcast_to(
            rate_ref[h : h + 1, begin + c * span : begin + (c + 1) * span], (span, span)
        ).T
        cumul = cumul_row.T
        decay = jnp.where(
            row_ids >= col_ids, jnp.exp(jnp.minimum(cumul - cumul_row, 0.0)), 0.0
        )
        return at, cumul, cumul_row, rate, decay

    lowers = []
    inverses = []
    for h, c in units:
        at, cumul, cumul_row, rate, decay = operands(h, c)
        keys = unit(proj_ref[(1,) + at])
        proj_ref[(1,) + at] = keys
        lower = jnp.where(row_ids > col_ids, rate * mm_nt(keys, keys) * decay, 0.0)
        lowers.append(lower)
        inverses.append(eye - jnp.where(row_ids >> 1 == col_ids >> 1, lower, 0.0))
    level = 1
    while (1 << level) < span:
        joins = (row_ids >> (level + 1) == col_ids >> (level + 1)) & (
            row_ids >> level != col_ids >> level
        )
        for u in range(len(units)):
            split = halves(inverses[u])
            inner = mm_split(halves(jnp.where(joins, lowers[u], 0.0)), split)
            inverses[u] = inverses[u] - mm_split(split, halves(inner))
        level += 1
    for h in range(heads):
        if first:
            carried = (
                lax.broadcasted_iota(jnp.int32, (width, 2 * width), 0)
                == lax.broadcasted_iota(jnp.int32, (width, 2 * width), 1)
            ).astype(f32)
        else:
            carried = carry_refs[0][h]
        for c in range(pieces):
            at, cumul, cumul_row, rate, decay = operands(h, c)
            keys = proj_ref[(1,) + at]
            queries = unit(proj_ref[(0,) + at])
            rate_col = rate[:, :1]
            growth = jnp.exp(cumul[:, :1])
            last = cumul_row[:1, span - 1 :]
            right_side = jnp.concatenate(
                [rate_col * growth * keys, rate_col * proj_ref[(2,) + at]], axis=1
            )
            solved = mm(inverses[h * pieces + c], right_side)
            mixed = mm(mm_nt(queries, keys) * decay, solved)
            tail = mm_tn(keys * jnp.exp(last - cumul[:, :1]), solved)
            entry = growth * queries - mixed[:, :width]
            reached = mm(entry, carried)
            rows_at = slice(c * span, (c + 1) * span)
            entry_ref[h, rows_at, :] = reached[:, :width].astype(bf16)
            local_ref[h, rows_at, :] = reached[:, width:] + mixed[:, width:]
            change = mm(tail[:, :width], carried)
            carried = jnp.exp(last) * carried - change
            carried = jnp.concatenate(
                [carried[:, :width], carried[:, width:] + tail[:, width:]], axis=1
            )
        map_ref[h] = carried.astype(map_ref.dtype)


def joined(maps, h, width):
    acc = maps[-1][h].astype(f32)
    for one in reversed(maps[:-1]):
        acc = mm(one[h, :, :width], acc)
        shift = one[h, :, width:].astype(f32)
        if acc.shape[1] == width:
            acc = acc + shift
        else:
            acc = jnp.concatenate([acc[:, :width], acc[:, width:] + shift], axis=1)
    return acc


def join_kernel(*refs):
    out_ref, shift_ref = refs[-2:]
    width = out_ref.shape[1]
    for h in range(out_ref.shape[0]):
        acc = joined(refs[:-2], h, width).astype(bf16)
        out_ref[h] = acc
        shift_ref[h] = acc[:, width:]


def heads_kernel(*refs, count, parts):
    map_refs = refs[:count]
    local_refs = refs[count : count + parts]
    entry_refs = refs[count + parts : count + 2 * parts]
    gain_ref = refs[count + 2 * parts]
    out_refs = refs[count + 2 * parts + 1 :]
    heads, _, width = local_refs[0].shape
    for h in range(heads):
        state = joined(map_refs, h, width)
        if state.shape[1] != width:
            state = state[:, width:]
        for part, out_ref in enumerate(out_refs):
            raw = local_refs[part][h] + mm(entry_refs[part][h], state)
            out_ref[:, h * width : (h + 1) * width] = (
                raw
                * lax.rsqrt(jnp.mean(raw * raw, axis=1, keepdims=True) + head_floor)
                * gain_ref[...]
            ).astype(bf16)


def back_kernel(*refs, peers):
    me_ref = refs[0]
    head_refs = refs[1 : 1 + peers]
    out_weight_refs = refs[1 + peers : 1 + 2 * peers]
    whole_ref, gain_ref, gate_ref, up_ref, down_ref = refs[1 + 2 * peers : 6 + 2 * peers]
    own_ref = refs[6 + 2 * peers]
    term_refs = refs[7 + 2 * peers : 7 + 3 * peers]
    residual_ref = refs[-1]
    me = me_ref[0]
    slice_width = own_ref.shape[1]
    attn = jnp.dot(head_refs[0][...], out_weight_refs[0][...], preferred_element_type=f32)
    for r in range(1, peers):
        attn = attn + jnp.dot(
            head_refs[r][...], out_weight_refs[r][...], preferred_element_type=f32
        )
    residual = whole_ref[...].astype(f32) + attn
    residual_ref[...] = residual
    normed = (
        residual
        * lax.rsqrt(jnp.mean(residual * residual, axis=1, keepdims=True) + norm_floor)
        * gain_ref[...]
    ).astype(bf16)
    gate = jnp.dot(normed, gate_ref[...], preferred_element_type=f32)
    up = jnp.dot(normed, up_ref[...], preferred_element_type=f32)
    hidden = (jax.nn.silu(gate) * up).astype(bf16)
    for r in reversed(range(peers)):
        at = pl.multiple_of((me ^ r) * slice_width, slice_width)
        term_refs[r][...] = jnp.dot(
            hidden, down_ref[:, pl.ds(at, slice_width)], preferred_element_type=f32
        ).astype(bf16)
    at = pl.multiple_of(me * slice_width, slice_width)
    own_ref[...] = residual_ref[:, pl.ds(at, slice_width)]


def call(kernel, outs, args, scratch=(), first_smem=True, flops=10**9, room=8):
    return pl.pallas_call(
        kernel,
        out_shape=[jax.ShapeDtypeStruct(s, d) for s, d in outs],
        in_specs=[smem if first_smem and i == 0 else vmem for i in range(len(args))],
        out_specs=[vmem] * len(outs),
        scratch_shapes=list(scratch),
        compiler_params=pltpu.CompilerParams(vmem_limit_bytes=room * mebi),
        cost_estimate=pl.CostEstimate(flops=flops, bytes_accessed=0, transcendentals=0),
    )(*args)


def shifted(x, axis, by):
    peers = lax.axis_size(axis)
    return lax.ppermute(x, axis, [(i, i + by) for i in range(peers - by)])


def earlier_maps(maps, axis):
    peers = lax.axis_size(axis)
    width = maps.shape[1]
    window = 1
    shift = None
    while window * radix < peers - 1:
        terms = [maps] + [shifted(maps, axis, window * k) for k in range(1, radix)]
        maps, shift = call(
            join_kernel,
            [(maps.shape, bf16), (maps.shape[:2] + (width,), bf16)],
            terms,
            first_smem=False,
        )
        window *= radix
    if shift is None:
        shift = maps[:, :, width:]
    offsets = list(range(1, peers, window))
    moved = [shifted(maps, axis, by) for by in offsets[:-1]]
    return moved + [shifted(shift, axis, by) for by in offsets[-1:]]


def body(
    layer_in,
    attn_gain,
    qkv_weight,
    log_decay,
    write_rate,
    head_gain,
    out_weight,
    ffn_gain,
    gate_weight,
    up_weight,
    down_weight,
):
    length, slice_width = layer_in.shape
    width = head_gain.shape[0]
    local_heads = qkv_weight.shape[2] // width
    model = attn_gain.shape[0]
    peers = lax.axis_size("tp")
    me = lax.axis_index("tp").astype(jnp.int32).reshape(1)
    parts = parts_of_block
    rows = length // parts
    span = min(128, rows)
    pieces = []
    for part in range(parts):
        cross = swap
        shard = lax.slice_in_dim(layer_in, part * rows, (part + 1) * rows)
        pieces.append(gather_pieces(shard, "tp", cross(shard, "tp", peers // 2)))
    held = lax.optimization_barrier((out_weight, pieces[-1][peers // 2]))[0]
    weight_far = swap(held, "tp", peers // 2)
    wholes, locals_, entries = [], [], []
    carried = ()
    for part in range(parts):
        last = part == parts - 1
        front = call
        whole, local, entry, maps = front(
            functools.partial(
                front_kernel,
                peers=peers,
                heads=local_heads,
                span=span,
                part=part,
                first=part == 0,
            ),
            [
                ((rows, model), bf16),
                ((local_heads, rows, width), f32),
                ((local_heads, rows, width), bf16),
                ((local_heads, width, 2 * width), bf16 if last else f32),
            ],
            [
                me,
                *pieces[part],
                attn_gain.reshape(1, model),
                qkv_weight,
                log_decay,
                write_rate,
                *carried,
            ],
            scratch=[pltpu.VMEM((3, rows, local_heads * width), f32)],
            flops=8 * 10**9,
            room=20,
        )
        carried = (maps,)
        wholes.append(whole)
        locals_.append(local)
        entries.append(entry)
    before = earlier_maps(maps, "seq")
    heads_out = call(
        functools.partial(heads_kernel, count=len(before), parts=parts),
        [((rows, local_heads * width), bf16)] * parts,
        [*before, *locals_, *entries, head_gain.reshape(1, width)],
        first_smem=False,
        flops=3 * 10**9,
    )
    weight_far, out_held, *heads_out = lax.optimization_barrier(
        (weight_far, out_weight, *heads_out)
    )
    weight_pieces = gather_pieces(out_held, "tp", weight_far)
    results = []
    gathered = []
    for shard in heads_out:
        lead = swap
        gathered.append(gather_pieces(shard, "tp", lead(shard, "tp", peers // 2)))
    for part in range(parts):
        back = call
        far = scatter_far
        own, *terms = back(
            functools.partial(back_kernel, peers=peers),
            [((rows, slice_width), f32)] + [((rows, slice_width), bf16)] * peers,
            [
                me,
                *gathered[part],
                *weight_pieces,
                wholes[part],
                ffn_gain.reshape(1, model),
                gate_weight,
                up_weight,
                down_weight,
            ],
            scratch=[pltpu.VMEM((rows, model), f32)],
            flops=6 * 10**9,
            room=28,
        )
        terms = scatter_near(dict(enumerate(terms)), "tp")
        if part + 1 < parts:
            gathered[part + 1], terms = lax.optimization_barrier((gathered[part + 1], terms))
        shared = far(terms, "tp")
        results.append((own + shared).astype(bf16))
    return jnp.concatenate(results, axis=0)


def solution(mesh):
    placed = (
        P("seq", "tp"),
        P(),
        P(None, None, "tp"),
        P("tp", "seq"),
        P("tp", "seq"),
        P(),
        P("tp", None),
        P(),
        P(None, "tp"),
        P(None, "tp"),
        P("tp", None),
    )
    return jax.shard_map(
        body, mesh=mesh, in_specs=placed, out_specs=P("seq", "tp"), check_vma=False
    )
```
